256 devices in a mesh: grp: 16 (over y, z_hi, core), dp: 16 (over z_lo, x).
Axes of the slice: x: 4, y: 4, z: 8 (z_hi: 2, z_lo: 4; z = z_hi * 4 + z_lo), core: 2. Of those that a mesh axis runs over, the one named last changes fastest.
Arguments:
- tokens: bfloat16 [16, 2048, 2048], P('grp', 'dp'), may hold values from -6 to 6
- hidden_grad: bfloat16 [16, 2048, 6144], P('grp', 'dp'), may hold values from -6 to 6
- w_gate: bfloat16 [16, 2048, 6144], P('grp', None, 'dp'), may hold values from -6 to 6
- w_up: bfloat16 [16, 2048, 6144], P('grp', None, 'dp'), may hold values from -6 to 6
Outputs:
- mixed_gate: bfloat16 [16, 2048, 6144], P('grp', None, 'dp')
- mixed_up: bfloat16 [16, 2048, 6144], P('grp', None, 'dp')
The draws below stay inside these ranges and needn't reach their ends.
All inputs are finite; a program needn't handle non-finite values.
Results may differ from the reference program's by a relative error of at most 0.0052.
Values may be sent and summed in bfloat16 or wider, within the bound.
No kernel may reach another device: no remote copies, remote signals or barrier semaphores. Data moves between devices by JAX's collectives and lax.ppermute only.
A program may use at most 256 MiB of HBM per device.

```python
import jax
import jax.numpy as jnp
from jax import lax

D = 2048
FF = 6144
GROUPS = 16
GROUP_TOKENS = 2048


def level_of(rng, shape, cuts, smallest, high):
    def one(axis_at, parts):
        heights = jax.random.uniform(jax.random.fold_in(jax.random.fold_in(rng, 6), axis_at), (parts,), jnp.float32, smallest / len(cuts), high / len(cuts))
        return jnp.repeat(jnp.exp(heights), shape[axis_at] // parts).reshape((-1,) + (1,) * (len(shape) - axis_at - 1))

    loudness = one(*cuts[0])
    for cut in cuts[1:]:
        loudness = loudness * one(*cut)
    return loudness


def scatter_about(key, dims, spread, reach, cuts=(), kind=jnp.bfloat16):
    drawn = jax.random.normal(key, dims, jnp.float32) * spread
    if len(cuts) > 0:
        drawn = level_of(key, dims, cuts, -0.22, 0.18) * drawn
    return jnp.clip(drawn, min=-reach, max=reach).astype(kind)


def setup_inputs(seed: int = 0) -> dict:
    key_of = jax.random.split(jax.random.key(seed), 5)
    tokens = scatter_about(key_of[0], (GROUPS, GROUP_TOKENS, D), 1.0, 6.0, ((0, 16), (1, 16)))
    hidden_grad = scatter_about(key_of[1], (GROUPS, GROUP_TOKENS, FF), 1.0, 6.0, ((0, 16), (1, 16)))
    w_gate = scatter_about(key_of[2], (GROUPS, D, FF), 1.0, 6.0, ((0, 16), (2, 16)))
    w_up = scatter_about(key_of[3], (GROUPS, D, FF), 1.0, 6.0, ((0, 16), (2, 16)))
    return dict(tokens=tokens, hidden_grad=hidden_grad, w_gate=w_gate, w_up=w_up)


def one_replica(operands):
    rows, cotangent, gate_weight, up_weight = operands
    scale = D ** -0.5
    gate = jnp.dot(rows, gate_weight, preferred_element_type=jnp.float32) * scale
    up = jnp.dot(rows, up_weight, preferred_element_type=jnp.float32) * scale
    sigma = jax.nn.sigmoid(gate)
    upstream = cotangent.astype(jnp.float32)
    gate_rows = (upstream * up * sigma * (1.0 + gate * (1.0 - sigma))).astype(jnp.bfloat16)
    up_rows = (upstream * gate * sigma).astype(jnp.bfloat16)
    gate_grad = jnp.dot(rows.T, gate_rows, preferred_element_type=jnp.float32) * scale
    up_grad = jnp.dot(rows.T, up_rows, preferred_element_type=jnp.float32) * scale
    gate_step = (gate_weight.astype(jnp.float32) - 0.5 * gate_grad).astype(jnp.bfloat16)
    up_step = (up_weight.astype(jnp.float32) - 0.5 * up_grad).astype(jnp.bfloat16)
    return gate_step, up_step


def average_cycle(stepped):
    wide = stepped.astype(jnp.float32)
    mixed = 0.5 * wide + 0.25 * (jnp.roll(wide, 1, axis=0) + jnp.roll(wide, -1, axis=0))
    return mixed.astype(jnp.bfloat16)


def reference(tokens, hidden_grad, w_gate, w_up):
    gate_step, up_step = lax.map(one_replica, (tokens, hidden_grad, w_gate, w_up))
    return average_cycle(gate_step), average_cycle(up_step)
```

```python
import jax
import jax.numpy as jnp
from jax import lax
from jax.sharding import PartitionSpec as P


NZ = 4
NX = 4


def ring_z(by):
    return [(z * NX + x, ((z + by) % NZ) * NX + x) for z in range(NZ) for x in range(NX)]


def ring_x(by):
    return [(z * NX + x, z * NX + (x + by) % NX) for z in range(NZ) for x in range(NX)]


def grp_ring(by):
    return [(i, (i + by) % 16) for i in range(16)]


def local(tokens, hidden_grad, w_gate, w_up):
    own = tokens[0]
    gate_weight = w_gate[0]
    up_weight = w_up[0]
    rows_local, width = own.shape
    units = gate_weight.shape[1]
    scale = width ** (-0.5)
    half = rows_local // 2
    dp = lax.axis_index("dp")
    z, x = dp // NX, dp % NX

    cot = lax.all_to_all(hidden_grad[0], "dp", split_axis=1, concat_axis=0, tiled=True)
    cot = cot.reshape(NZ * NX, rows_local, units)

    def cot_block(dz, dx):
        at = ((z - dz) % NZ) * NX + (x - dx) % NX
        return lax.dynamic_index_in_dim(cot, at, 0, keepdims=False)

    acc = None
    cur = own
    for k in range(NZ):
        a = lax.ppermute(cur, "dp", ring_x(1))
        b = lax.ppermute(cur, "dp", ring_x(-1))
        nxt = lax.ppermute(cur, "dp", ring_z(1)) if k + 1 < NZ else None
        c1 = lax.ppermute(a[:half], "dp", ring_x(1))
        c2 = lax.ppermute(b[half:], "dp", ring_x(-1))
        rows = jnp.concatenate([cur, a, b, c1, c2], axis=0)
        upstream = jnp.concatenate([cot_block(k, 0), cot_block(k, 1), cot_block(k, -1), cot_block(k, 2)], axis=0).astype(jnp.float32)
        gate = jnp.dot(rows, gate_weight, preferred_element_type=jnp.float32) * scale
        up = jnp.dot(rows, up_weight, preferred_element_type=jnp.float32) * scale
        sigma = jax.nn.sigmoid(gate)
        gate_rows = (upstream * up * sigma * (1.0 + gate * (1.0 - sigma))).astype(jnp.bfloat16)
        up_rows = (upstream * gate * sigma).astype(jnp.bfloat16)
        if k + 1 < NZ:
            both = jnp.concatenate([gate_rows, up_rows], axis=1)
            part = lax.dot_general(rows, both, (((0,), (0,)), ((), ())), preferred_element_type=jnp.float32)
            acc = part if acc is None else acc + part
            cur = nxt
        else:
            last = (rows, gate_rows, up_rows)

    rows, gate_rows, up_rows = last
    chunks = 3
    cw = units // chunks
    outs_g, outs_u = [], []
    sent = []
    for c in range(chunks):
        sl = slice(c * cw, (c + 1) * cw)
        both = jnp.concatenate([gate_rows[:, sl], up_rows[:, sl]], axis=1)
        part = lax.dot_general(rows, both, (((0,), (0,)), ((), ())), preferred_element_type=jnp.float32)
        base = jnp.concatenate([acc[:, sl], acc[:, units + c * cw: units + (c + 1) * cw]], axis=1)
        w = jnp.concatenate([gate_weight[:, sl], up_weight[:, sl]], axis=1).astype(jnp.float32)
        s = (w - 0.5 * ((base + part) * scale)).astype(jnp.bfloat16)
        left = lax.ppermute(s, "grp", grp_ring(1))
        right = lax.ppermute(s, "grp", grp_ring(-1))
        sent.append((s, left, right))
    for s, left, right in sent:
        m = 0.5 * s.astype(jnp.float32) + 0.25 * (left.astype(jnp.float32) + right.astype(jnp.float32))
        m = m.astype(jnp.bfloat16)
        outs_g.append(m[:, :cw])
        outs_u.append(m[:, cw:])
    return jnp.concatenate(outs_g, axis=1)[None], jnp.concatenate(outs_u, axis=1)[None]


def solution(mesh):
    in_specs = (
        P("grp", "dp", None),
        P("grp", "dp", None),
        P("grp", None, "dp"),
        P("grp", None, "dp"),
    )
    out_specs = (P("grp", None, "dp"), P("grp", None, "dp"))
    return jax.shard_map(local, mesh=mesh, in_specs=in_specs, out_specs=out_specs, check_vma=False)
```

```python
import functools

import jax
import jax.numpy as jnp
from jax import lax
from jax.experimental import pallas as pl
from jax.experimental.pallas import tpu as pltpu
from jax.sharding import PartitionSpec as P


NZ = 4
NX = 4
DX = (0, 1, -1, 2)
CHUNKS = 3
VMEM = pl.BlockSpec(memory_space=pltpu.VMEM)
SMEM = pl.BlockSpec(memory_space=pltpu.SMEM)
ANY = pl.BlockSpec(memory_space=pl.ANY)
HBM = pl.BlockSpec(memory_space=pltpu.HBM)
MIB = 1024 * 1024


def params(mib):
    return pltpu.CompilerParams(vmem_limit_bytes=mib * MIB)


def device_pairs(grp, move):
    out = []
    for g in range(grp):
        for z in range(NZ):
            for x in range(NX):
                to = move(g, z, x)
                if to is not None:
                    h, u, v = to
                    out.append(((g * NZ + z) * NX + x, ((h % grp) * NZ + u % NZ) * NX + v % NX))
    return out


def split_body(hg, *refs):
    out = refs[-1]
    units = out.shape[2]
    for i in range(out.shape[0]):
        out[i] = hg[:, i * units:(i + 1) * units]


def split_units(hg, parts, *deps):
    rows, width = hg.shape
    return pl.pallas_call(
        split_body,
        out_shape=jax.ShapeDtypeStruct((parts, rows, width // parts), hg.dtype),
        in_specs=[VMEM] + [HBM] * len(deps),
        out_specs=VMEM,
        compiler_params=params(8),
        name="split",
    )(hg, *deps)


def pack_body(g, u, out):
    uw = g.shape[1]
    out[0, :, :uw] = g[...]
    out[0, :, uw:] = u[...]


def pack_weights(g, u):
    width, units = g.shape
    uw = units // CHUNKS
    read = pl.BlockSpec((width, uw), lambda c: (0, c))
    return pl.pallas_call(
        pack_body,
        grid=(CHUNKS,),
        out_shape=jax.ShapeDtypeStruct((CHUNKS, width, 2 * uw), g.dtype),
        in_specs=[read, read],
        out_specs=pl.BlockSpec((1, width, 2 * uw), lambda c: (c, 0, 0)),
        compiler_params=params(10),
        name="pack",
    )(g, u)


def cat_body(count, *refs):
    xs, out, sems = refs[:count], refs[-2], refs[-1]
    copies, at = [], 0
    for i, v in enumerate(xs):
        copies.append(pltpu.make_async_copy(v, out.at[pl.ds(at, v.shape[0])], sems.at[i]))
        at += v.shape[0]
    for c in copies:
        c.start()
    for c in copies:
        c.wait()


def cat(xs, *deps):
    n = sum(v.shape[0] for v in xs)
    return pl.pallas_call(
        functools.partial(cat_body, len(xs)),
        out_shape=jax.ShapeDtypeStruct((n,) + xs[0].shape[1:], xs[0].dtype),
        in_specs=[HBM] * (len(xs) + len(deps)),
        out_specs=HBM,
        scratch_shapes=[pltpu.SemaphoreType.DMA((len(xs),))],
        compiler_params=params(4),
        name="cat",
    )(*xs, *deps)


def step_body(which, count, meta, hg, w, *refs):
    xs = refs[:count]
    rest = refs[count:]
    other = rest[0] if which == 1 else None
    out, x, rows, sems = rest[-4:]
    uw = w.shape[2] // 2
    blk = hg.shape[1]
    part = 512
    scale = w.shape[1] ** (-0.5)

    @pl.when(meta[0] == which)
    def _():
        at = 0
        for v in xs:
            pltpu.make_async_copy(v, x.at[pl.ds(at, v.shape[0])], sems.at[at // part]).start()
            at += v.shape[0]

        def products(i, carry):
            at = pl.multiple_of(i * part, part)
            here = x.at[pl.ds(at, part)]
            pltpu.make_async_copy(here, here, sems.at[i]).wait()
            gu = jnp.dot(x[pl.ds(at, part), :], w[0], preferred_element_type=jnp.float32) * scale
            for j in range(part // blk):
                gate = gu[j * blk:(j + 1) * blk, :uw]
                up = gu[j * blk:(j + 1) * blk, uw:]
                upstream = hg[meta[1 + i * (part // blk) + j]].astype(jnp.float32)
                sigma = jax.nn.sigmoid(gate)
                g = upstream * up * sigma * (1.0 + gate * (1.0 - sigma))
                u = upstream * gate * sigma
                to = pl.ds(pl.multiple_of(at + j * blk, blk), blk)
                rows[to, :uw] = g.astype(jnp.bfloat16)
                rows[to, uw:] = u.astype(jnp.bfloat16)
            return carry

        lax.fori_loop(0, x.shape[0] // part, products, 0)

        def band(i, carry):
            at = pl.multiple_of(i * part, part)
            grad = lax.dot_general(x[:, pl.ds(at, part)], rows[...], (((0,), (0,)), ((), ())), preferred_element_type=jnp.float32)
            old = w[0, pl.ds(at, part), :].astype(jnp.float32)
            out[pl.ds(at, part), :] = (old - 0.5 * (grad * scale)).astype(jnp.bfloat16)
            return carry

        lax.fori_loop(0, w.shape[1] // part, band, 0)

    if other is not None:
        @pl.when(meta[0] != which)
        def _():
            pltpu.sync_copy(other, out)


def step_chunk(which, c, meta, hg, w, xs, *extra):
    width = w.shape[1]
    n = sum(v.shape[0] for v in xs)
    both = w.shape[2]
    return pl.pallas_call(
        functools.partial(step_body, which, len(xs)),
        grid=(1,),
        out_shape=jax.ShapeDtypeStruct((width, both), jnp.bfloat16),
        in_specs=[
            SMEM,
            pl.BlockSpec(hg.shape[:2] + (both // 2,), lambda i: (0, 0, c)),
            pl.BlockSpec((1, width, both), lambda i: (c, 0, 0)),
        ]
        + [HBM] * (len(xs) + len(extra)),
        out_specs=pl.BlockSpec((width, both), lambda i: (0, 0)),
        scratch_shapes=[
            pltpu.VMEM((n, width), jnp.bfloat16),
            pltpu.VMEM((n, both), jnp.bfloat16),
            pltpu.SemaphoreType.DMA((n // 512,)),
        ],
        compiler_params=params(32),
        cost_estimate=pl.CostEstimate(flops=4 * n * width * both, bytes_accessed=n * width * 2, transcendentals=n * 128),
        name="step",
    )(meta, hg, w, *xs, *extra)


def mix_body(meta, own, near, far_a, far_b, *refs):
    og, ou = refs[-2:]
    uw = og.shape[1]
    f = jnp.float32

    def store(far):
        m = 0.5 * own[...].astype(f) + 0.25 * (near[...].astype(f) + far[...].astype(f))
        m = m.astype(jnp.bfloat16)
        og[...] = m[:, :uw]
        ou[...] = m[:, uw:]

    @pl.when(meta[0] == 0)
    def _():
        store(far_b)

    @pl.when(meta[0] == 1)
    def _():
        store(far_a)


def mix_chunk(c, meta, own, near, far_a, far_b, done):
    width, both = own.shape
    uw = both // 2
    band = 512
    read = pl.BlockSpec((band, both), lambda i: (i, 0))
    write = pl.BlockSpec((band, uw), lambda i: (i, c))
    extra = [] if done is None else list(done)
    return pl.pallas_call(
        mix_body,
        grid=(width // band,),
        out_shape=(jax.ShapeDtypeStruct((width, CHUNKS * uw), jnp.bfloat16),) * 2,
        in_specs=[SMEM] + [read] * 4 + [ANY] * len(extra),
        out_specs=(write, write),
        input_output_aliases={} if done is None else {5: 0, 6: 1},
        compiler_params=params(10),
        name="mix",
    )(meta, own, near, far_a, far_b, *extra)


def local(tokens, hidden_grad, w_gate, w_up):
    axes = ("grp", "dp")
    groups = lax.axis_size("grp")
    own = tokens[0]
    dp = lax.axis_index("dp")
    core = lax.axis_index("grp") % 2
    z, x = dp // NX, dp % NX

    def send(v, move):
        return lax.ppermute(v, axes, device_pairs(groups, move))

    def along_x(v, which, by):
        return send(v, lambda g, u, t: (g, u, t + by) if g % 2 == which else None)

    def table(pairs):
        up = jnp.array([k for k, d in pairs], jnp.int32)
        along = jnp.array([d for k, d in pairs], jnp.int32)
        src = ((z + NZ - up) % NZ) * NX + (x + NX - along) % NX
        return jnp.concatenate([core.reshape(1), src]).astype(jnp.int32)

    halves = ((0, 1), (2, 3))
    meta_a = table([(k, d) for h in halves for d in DX for k in h])
    meta_b = table([(k, d) for d in DX for k in range(NZ)])

    def ahead_by(v):
        return send(v, lambda g, u, t: (g, u + 1, t))

    def fan(v, which):
        out = [v]
        for d in DX[1:]:
            out.append(along_x(v, which, d))
        return out

    def swap(v):
        return send(v, lambda g, u, t: (g + 1 - 2 * (g % 2), u, t))

    w = pack_weights(w_gate[0], w_up[0])
    r1 = ahead_by(own)
    r2 = ahead_by(r1)
    first = cat([own, r1])
    ahead = fan(first, 0)
    r3 = ahead_by(r2)
    hg = split_units(hidden_grad[0], NZ * NX, r2)
    hg = lax.all_to_all(hg, "dp", split_axis=0, concat_axis=0, tiled=True)
    second = cat([r2, r3])
    behind = fan(second, 0)

    step_a, cross_a = [], []
    for c in range(CHUNKS):
        step_a.append(step_chunk(0, c, meta_a, hg, w, ahead + behind))
        cross_a.append(send(step_a[c], lambda g, u, t: (g - 1, u, t) if g % 2 == 0 else None))

    token = swap(step_a[0][:8, :128])
    block = cat([first, second], token, *step_a)
    blocks = fan(block, 1)
    mine, cross_b, near = [], [], []
    for c in range(CHUNKS):
        mine.append(step_chunk(1, c, meta_b, hg, w, blocks, step_a[c]))
        cross_b.append(send(mine[c], lambda g, u, t: (g + 1, u, t) if g % 2 == 1 else None))
        near.append(swap(mine[c]))

    done = None
    for c in range(CHUNKS):
        done = mix_chunk(c, meta_a, mine[c], near[c], cross_a[c], cross_b[c], done)
    return done[0][None], done[1][None]


def solution(mesh):
    in_specs = (
        P("grp", "dp", None),
        P("grp", "dp", None),
        P("grp", None, "dp"),
        P("grp", None, "dp"),
    )
    out_specs = (P("grp", None, "dp"), P("grp", None, "dp"))

    return jax.shard_map(local, mesh=mesh, in_specs=in_specs, out_specs=out_specs, check_vma=False)
```

```python
import functools

import jax
import jax.numpy as jnp
from jax import lax
from jax.experimental import pallas as pl
from jax.experimental.pallas import tpu as pltpu
from jax.sharding import PartitionSpec as P


NZ = 4
NX = 4
DX = (0, 1, -1, 2)
CHUNKS = 3
VMEM = pl.BlockSpec(memory_space=pltpu.VMEM)
SMEM = pl.BlockSpec(memory_space=pltpu.SMEM)
ANY = pl.BlockSpec(memory_space=pl.ANY)
HBM = pl.BlockSpec(memory_space=pltpu.HBM)
MIB = 1024 * 1024


def params(mib):
    return pltpu.CompilerParams(vmem_limit_bytes=mib * MIB)


def device_pairs(grp, move):
    out = []
    for g in range(grp):
        for z in range(NZ):
            for x in range(NX):
                to = move(g, z, x)
                if to is not None:
                    h, u, v = to
                    out.append(((g * NZ + z) * NX + x, ((h % grp) * NZ + u % NZ) * NX + v % NX))
    return out


def split_body(hg, out, sem):
    units = out.shape[2]
    for i in range(out.shape[0]):
        pltpu.make_async_copy(hg.at[:, i * units:(i + 1) * units], out.at[i], sem.at[i]).start()
    for i in range(out.shape[0]):
        pltpu.make_async_copy(hg.at[:, i * units:(i + 1) * units], out.at[i], sem.at[i]).wait()


def split_units(hg, parts):
    rows, width = hg.shape
    return pl.pallas_call(
        split_body,
        out_shape=jax.ShapeDtypeStruct((parts, rows, width // parts), hg.dtype),
        in_specs=[HBM],
        out_specs=HBM,
        scratch_shapes=[pltpu.SemaphoreType.DMA((parts,))],
        compiler_params=params(4),
        name="split",
    )(hg)


def pack_body(g, u, out):
    uw = g.shape[1]
    out[0, :, :uw] = g[...]
    out[0, :, uw:] = u[...]


def pack_weights(g, u):
    width, units = g.shape
    uw = units // CHUNKS
    read = pl.BlockSpec((width, uw), lambda c: (0, c))
    return pl.pallas_call(
        pack_body,
        grid=(CHUNKS,),
        out_shape=jax.ShapeDtypeStruct((CHUNKS, width, 2 * uw), g.dtype),
        in_specs=[read, read],
        out_specs=pl.BlockSpec((1, width, 2 * uw), lambda c: (c, 0, 0)),
        compiler_params=params(10),
        name="pack",
    )(g, u)


def pick_body(meta, own, got, a, b, sems):
    half = a.shape[0]
    for core in range(2):
        @pl.when(meta[0] == core)
        def _():
            at = pl.ds(core * half, half)
            ca = pltpu.make_async_copy((own if core == 0 else got).at[at], a, sems.at[0])
            cb = pltpu.make_async_copy((got if core == 0 else own).at[at], b, sems.at[1])
            ca.start()
            cb.start()
            ca.wait()
            cb.wait()


def pick(meta, own, got):
    shape = jax.ShapeDtypeStruct((own.shape[0] // 2, own.shape[1]), own.dtype)
    return pl.pallas_call(
        pick_body,
        out_shape=(shape, shape),
        in_specs=[SMEM, HBM, HBM],
        out_specs=(HBM, HBM),
        scratch_shapes=[pltpu.SemaphoreType.DMA((2,))],
        compiler_params=params(4),
        name="pick",
    )(meta, own, got)


def cat_body(count, *refs):
    xs, out, sems = refs[:count], refs[-2], refs[-1]
    copies, at = [], 0
    for i, v in enumerate(xs):
        copies.append(pltpu.make_async_copy(v, out.at[pl.ds(at, v.shape[0])], sems.at[i]))
        at += v.shape[0]
    for c in copies:
        c.start()
    for c in copies:
        c.wait()


def cat(xs, *deps):
    n = sum(v.shape[0] for v in xs)
    return pl.pallas_call(
        functools.partial(cat_body, len(xs)),
        out_shape=jax.ShapeDtypeStruct((n,) + xs[0].shape[1:], xs[0].dtype),
        in_specs=[HBM] * (len(xs) + len(deps)),
        out_specs=HBM,
        scratch_shapes=[pltpu.SemaphoreType.DMA((len(xs),))],
        compiler_params=params(4),
        name="cat",
    )(*xs, *deps)


def step_body(which, count, c, meta, units, packed, *refs):
    xs = refs[:count]
    rest = refs[count:]
    other = rest[0] if which == 1 else None
    out, x, w, hg, rows, sems = rest[-6:]
    uw = w.shape[1] // 2
    blk = hg.shape[1] // 2
    part = 512
    scale = w.shape[0] ** (-0.5)

    @pl.when(meta[0] == which)
    def _():
        weights = pltpu.make_async_copy(packed.at[c], w, sems.at[x.shape[0] // part])
        weights.start()
        cotangents = pltpu.make_async_copy(units.at[:, :, c * uw:(c + 1) * uw], hg, sems.at[x.shape[0] // part + 1])
        cotangents.start()
        at = 0
        for v in xs:
            done = 0
            while done < v.shape[0]:
                n = min(part - at % part, v.shape[0] - done)
                pltpu.make_async_copy(v.at[pl.ds(done, n)], x.at[pl.ds(at, n)], sems.at[at // part]).start()
                at += n
                done += n
        weights.wait()
        cotangents.wait()

        def products(i, carry):
            at = pl.multiple_of(i * part, part)
            here = x.at[pl.ds(at, part)]
            pltpu.make_async_copy(here, here, sems.at[i]).wait()
            half = pl.multiple_of(jnp.where(i < 2, which, 1 - which) * blk, blk)
            gu = jnp.dot(x[pl.ds(at, part), :], w[...], preferred_element_type=jnp.float32) * scale
            for j in range(part // blk):
                gate = gu[j * blk:(j + 1) * blk, :uw]
                up = gu[j * blk:(j + 1) * blk, uw:]
                upstream = hg[meta[1 + (i % 2) * (part // blk) + j], pl.ds(half, blk), :].astype(jnp.float32)
                sigma = jax.nn.sigmoid(gate)
                g = upstream * up * sigma * (1.0 + gate * (1.0 - sigma))
                u = upstream * gate * sigma
                to = pl.ds(pl.multiple_of(at + j * blk, blk), blk)
                rows[to, :uw] = g.astype(jnp.bfloat16)
                rows[to, uw:] = u.astype(jnp.bfloat16)
            return carry

        lax.fori_loop(0, x.shape[0] // part, products, 0)

        def band(i, carry):
            at = pl.multiple_of(i * part, part)
            grad = lax.dot_general(x[:, pl.ds(at, part)], rows[...], (((0,), (0,)), ((), ())), preferred_element_type=jnp.float32)
            old = w[pl.ds(at, part), :].astype(jnp.float32)
            out[pl.ds(at, part), :] = (old - 0.5 * (grad * scale)).astype(jnp.bfloat16)
            return carry

        lax.fori_loop(0, w.shape[0] // part, band, 0)

    if other is not None:
        @pl.when(meta[0] != which)
        def _():
            pltpu.sync_copy(other, out)


def step_chunk(which, c, meta, hg, w, xs, *extra):
    width = w.shape[1]
    n = sum(v.shape[0] for v in xs)
    both = w.shape[2]
    return pl.pallas_call(
        functools.partial(step_body, which, len(xs), c),
        grid=(1,),
        out_shape=jax.ShapeDtypeStruct((width, both), jnp.bfloat16),
        in_specs=[SMEM] + [HBM] * (2 + len(xs) + len(extra)),
        out_specs=pl.BlockSpec((width, both), lambda i: (0, 0)),
        scratch_shapes=[
            pltpu.VMEM((n, width), jnp.bfloat16),
            pltpu.VMEM((width, both), jnp.bfloat16),
            pltpu.VMEM(hg.shape[:2] + (both // 2,), jnp.bfloat16),
            pltpu.VMEM((n, both), jnp.bfloat16),
            pltpu.SemaphoreType.DMA((n // 512 + 2,)),
        ],
        compiler_params=params(32),
        cost_estimate=pl.CostEstimate(flops=4 * n * width * both, bytes_accessed=n * width * 2, transcendentals=n * 128),
        name="step",
    )(meta, hg, w, *xs, *extra)


def mix_body(meta, own, near, far_a, far_b, *refs):
    og, ou = refs[-2:]
    uw = og.shape[1]
    f = jnp.float32

    def store(far):
        m = 0.5 * own[...].astype(f) + 0.25 * (near[...].astype(f) + far[...].astype(f))
        m = m.astype(jnp.bfloat16)
        og[...] = m[:, :uw]
        ou[...] = m[:, uw:]

    @pl.when(meta[0] == 0)
    def _():
        store(far_b)

    @pl.when(meta[0] == 1)
    def _():
        store(far_a)


def mix_chunk(c, meta, own, near, far_a, far_b, done):
    width, both = own.shape
    uw = both // 2
    band = 512
    read = pl.BlockSpec((band, both), lambda i: (i, 0))
    write = pl.BlockSpec((band, uw), lambda i: (i, c))
    extra = [] if done is None else list(done)
    return pl.pallas_call(
        mix_body,
        grid=(width // band,),
        out_shape=(jax.ShapeDtypeStruct((width, CHUNKS * uw), jnp.bfloat16),) * 2,
        in_specs=[SMEM] + [read] * 4 + [ANY] * len(extra),
        out_specs=(write, write),
        input_output_aliases={} if done is None else {5: 0, 6: 1},
        compiler_params=params(10),
        name="mix",
    )(meta, own, near, far_a, far_b, *extra)


def local(tokens, hidden_grad, w_gate, w_up):
    axes = ("grp", "dp")
    groups = lax.axis_size("grp")
    own = tokens[0]
    dp = lax.axis_index("dp")
    core = lax.axis_index("grp") % 2
    z, x = dp // NX, dp % NX

    def send(v, move):
        return lax.ppermute(v, axes, device_pairs(groups, move))

    def along_x(v, by):
        return send(v, lambda g, u, t: (g, u, t + by))

    def along_z(v, by):
        return send(v, lambda g, u, t: (g, u + by, t))

    def table(pairs):
        up = jnp.array([k for k, d in pairs], jnp.int32)
        along = jnp.array([d for k, d in pairs], jnp.int32)
        src = ((z + NZ - up) % NZ) * NX + (x + NX - along) % NX
        return jnp.concatenate([core.reshape(1), src]).astype(jnp.int32)

    meta_a = table([(k, d) for k in range(NZ) for d in DX])
    meta_b = table([(k, d) for d in DX for k in range(NZ)])

    def fan(v):
        out = [v]
        for d in DX[1:]:
            out.append(along_x(v, d))
        return out

    def swap(v):
        return send(v, lambda g, u, t: (g + 1 - 2 * (g % 2), u, t))

    half_a, half_b = pick(meta_a, own, swap(own))
    w = pack_weights(w_gate[0], w_up[0])
    r1 = along_z(half_a, 1)
    own_a = fan(half_a)
    r2 = along_z(r1, 1)
    one_a = fan(r1)
    r3 = along_z(r2, 1)
    two_a = fan(r2)
    hg = split_units(hidden_grad[0], NZ * NX)
    hg = lax.all_to_all(hg, "dp", split_axis=0, concat_axis=0, tiled=True)
    three_a = fan(r3)
    column_b = [along_z(half_b, k) for k in range(1, NZ)]
    early = cat(own_a + one_a + two_a)
    late = cat(three_a)
    pieces = [early, late, swap(early), swap(late)]

    step_a, cross_a = [], []
    for c in range(CHUNKS):
        step_a.append(step_chunk(0, c, meta_a, hg, w, pieces))
        cross_a.append(send(step_a[c], lambda g, u, t: (g - 1, u, t) if g % 2 == 0 else None))

    blocks = cat(fan(cat([half_b] + column_b, step_a[0])))
    blocks = [blocks, swap(blocks)]
    mine, cross_b, near = [], [], []
    for c in range(CHUNKS):
        mine.append(step_chunk(1, c, meta_b, hg, w, blocks, step_a[c]))
        cross_b.append(send(mine[c], lambda g, u, t: (g + 1, u, t) if g % 2 == 1 else None))
        near.append(swap(mine[c]))

    done = None
    for c in range(CHUNKS):
        done = mix_chunk(c, meta_a, mine[c], near[c], cross_a[c], cross_b[c], done)
    return done[0][None], done[1][None]


def solution(mesh):
    in_specs = (
        P("grp", "dp", None),
        P("grp", "dp", None),
        P("grp", None, "dp"),
        P("grp", None, "dp"),
    )
    out_specs = (P("grp", None, "dp"), P("grp", None, "dp"))

    return jax.shard_map(local, mesh=mesh, in_specs=in_specs, out_specs=out_specs, check_vma=False)
```

```python
import functools

import jax
import jax.numpy as jnp
from jax import lax
from jax.experimental import pallas as pl
from jax.experimental.pallas import tpu as pltpu
from jax.sharding import PartitionSpec as P


NZ = 4
NX = 4
DX = (0, 1, -1, 2)
CHUNKS = 3
VMEM = pl.BlockSpec(memory_space=pltpu.VMEM)
SMEM = pl.BlockSpec(memory_space=pltpu.SMEM)
ANY = pl.BlockSpec(memory_space=pl.ANY)
HBM = pl.BlockSpec(memory_space=pltpu.HBM)
MIB = 1024 * 1024


def params(mib):
    return pltpu.CompilerParams(vmem_limit_bytes=mib * MIB)


def device_pairs(grp, move):
    out = []
    for g in range(grp):
        for z in range(NZ):
            for x in range(NX):
                to = move(g, z, x)
                if to is not None:
                    h, u, v = to
                    out.append(((g * NZ + z) * NX + x, ((h % grp) * NZ + u % NZ) * NX + v % NX))
    return out


def split_body(hg, out, sem):
    units = out.shape[2]
    for i in range(out.shape[0]):
        pltpu.make_async_copy(hg.at[:, i * units:(i + 1) * units], out.at[i], sem.at[i]).start()
    for i in range(out.shape[0]):
        pltpu.make_async_copy(hg.at[:, i * units:(i + 1) * units], out.at[i], sem.at[i]).wait()


def split_units(hg, parts):
    rows, width = hg.shape
    return pl.pallas_call(
        split_body,
        out_shape=jax.ShapeDtypeStruct((parts, rows, width // parts), hg.dtype),
        in_specs=[HBM],
        out_specs=HBM,
        scratch_shapes=[pltpu.SemaphoreType.DMA((parts,))],
        compiler_params=params(4),
        name="split",
    )(hg)


def pack_body(g, u, out):
    uw = g.shape[1]
    out[0, :, :uw] = g[...]
    out[0, :, uw:] = u[...]


def pack_weights(g, u):
    width, units = g.shape
    uw = units // CHUNKS
    read = pl.BlockSpec((width, uw), lambda c: (0, c))
    return pl.pallas_call(
        pack_body,
        grid=(CHUNKS,),
        out_shape=jax.ShapeDtypeStruct((CHUNKS, width, 2 * uw), g.dtype),
        in_specs=[read, read],
        out_specs=pl.BlockSpec((1, width, 2 * uw), lambda c: (c, 0, 0)),
        compiler_params=params(10),
        name="pack",
    )(g, u)


def pick_body(meta, own, got, a, b, sems):
    half = a.shape[0]
    for core in range(2):
        @pl.when(meta[0] == core)
        def _():
            at = pl.ds(core * half, half)
            ca = pltpu.make_async_copy((own if core == 0 else got).at[at], a, sems.at[0])
            cb = pltpu.make_async_copy((got if core == 0 else own).at[at], b, sems.at[1])
            ca.start()
            cb.start()
            ca.wait()
            cb.wait()


def pick(meta, own, got):
    shape = jax.ShapeDtypeStruct((own.shape[0] // 2, own.shape[1]), own.dtype)
    return pl.pallas_call(
        pick_body,
        out_shape=(shape, shape),
        in_specs=[SMEM, HBM, HBM],
        out_specs=(HBM, HBM),
        scratch_shapes=[pltpu.SemaphoreType.DMA((2,))],
        compiler_params=params(4),
        name="pick",
    )(meta, own, got)


def cat_body(count, *refs):
    xs, out, sems = refs[:count], refs[-2], refs[-1]
    copies, at = [], 0
    for i, v in enumerate(xs):
        copies.append(pltpu.make_async_copy(v, out.at[pl.ds(at, v.shape[0])], sems.at[i]))
        at += v.shape[0]
    for c in copies:
        c.start()
    for c in copies:
        c.wait()


def cat(xs, *deps):
    n = sum(v.shape[0] for v in xs)
    return pl.pallas_call(
        functools.partial(cat_body, len(xs)),
        out_shape=jax.ShapeDtypeStruct((n,) + xs[0].shape[1:], xs[0].dtype),
        in_specs=[HBM] * (len(xs) + len(deps)),
        out_specs=HBM,
        scratch_shapes=[pltpu.SemaphoreType.DMA((len(xs),))],
        compiler_params=params(4),
        name="cat",
    )(*xs, *deps)


def step_body(which, count, c, meta, units, packed, *refs):
    xs = refs[:count]
    rest = refs[count:]
    other = rest[0] if which == 1 else None
    out, x, w, hg, rows, sems = rest[-6:]
    uw = w.shape[1] // 2
    blk = hg.shape[1] // 2
    part = 512
    scale = w.shape[0] ** (-0.5)

    @pl.when(meta[0] == which)
    def _():
        weights = pltpu.make_async_copy(packed.at[c], w, sems.at[x.shape[0] // part])
        weights.start()
        cotangents = pltpu.make_async_copy(units.at[:, :, c * uw:(c + 1) * uw], hg, sems.at[x.shape[0] // part + 1])
        cotangents.start()
        at = 0
        for v in xs:
            done = 0
            while done < v.shape[0]:
                n = min(part - at % part, v.shape[0] - done)
                pltpu.make_async_copy(v.at[pl.ds(done, n)], x.at[pl.ds(at, n)], sems.at[at // part]).start()
                at += n
                done += n
        weights.wait()
        cotangents.wait()

        def products(i, carry):
            at = pl.multiple_of(i * part, part)
            here = x.at[pl.ds(at, part)]
            pltpu.make_async_copy(here, here, sems.at[i]).wait()
            half = pl.multiple_of(jnp.where(i < 2, which, 1 - which) * blk, blk)
            gu = jnp.dot(x[pl.ds(at, part), :], w[...], preferred_element_type=jnp.float32) * scale
            for j in range(part // blk):
                gate = gu[j * blk:(j + 1) * blk, :uw]
                up = gu[j * blk:(j + 1) * blk, uw:]
                upstream = hg[meta[1 + (i % 2) * (part // blk) + j], pl.ds(half, blk), :].astype(jnp.float32)
                sigma = jax.nn.sigmoid(gate)
                g = upstream * up * sigma * (1.0 + gate * (1.0 - sigma))
                u = upstream * gate * sigma
                to = pl.ds(pl.multiple_of(at + j * blk, blk), blk)
                rows[to, :uw] = g.astype(jnp.bfloat16)
                rows[to, uw:] = u.astype(jnp.bfloat16)
            return carry

        lax.fori_loop(0, x.shape[0] // part, products, 0)

        def band(i, carry):
            at = pl.multiple_of(i * part, part)
            grad = lax.dot_general(x[:, pl.ds(at, part)], rows[...], (((0,), (0,)), ((), ())), preferred_element_type=jnp.float32)
            old = w[pl.ds(at, part), :].astype(jnp.float32)
            out[pl.ds(at, part), :] = (old - 0.5 * (grad * scale)).astype(jnp.bfloat16)
            return carry

        lax.fori_loop(0, w.shape[0] // part, band, 0)

    @pl.when(meta[0] != which)
    def _():
        if other is None:
            out[...] = jnp.zeros(out.shape, out.dtype)
        else:
            pltpu.sync_copy(other, out)


def step_chunk(which, c, meta, hg, w, xs, *extra):
    width = w.shape[1]
    n = sum(v.shape[0] for v in xs)
    both = w.shape[2]
    return pl.pallas_call(
        functools.partial(step_body, which, len(xs), c),
        grid=(1,),
        out_shape=jax.ShapeDtypeStruct((width, both), jnp.bfloat16),
        in_specs=[SMEM] + [HBM] * (2 + len(xs) + len(extra)),
        out_specs=pl.BlockSpec((width, both), lambda i: (0, 0)),
        scratch_shapes=[
            pltpu.VMEM((n, width), jnp.bfloat16),
            pltpu.VMEM((width, both), jnp.bfloat16),
            pltpu.VMEM(hg.shape[:2] + (both // 2,), jnp.bfloat16),
            pltpu.VMEM((n, both), jnp.bfloat16),
            pltpu.SemaphoreType.DMA((n // 512 + 2,)),
        ],
        compiler_params=params(32),
        cost_estimate=pl.CostEstimate(flops=4 * n * width * both, bytes_accessed=n * width * 2, transcendentals=n * 128),
        name="step",
    )(meta, hg, w, *xs, *extra)


def mix_body(meta, own, near, far_a, far_b, *refs):
    og, ou = refs[-2:]
    uw = og.shape[1]
    f = jnp.float32

    def store(far):
        m = 0.5 * own[...].astype(f) + 0.25 * (near[...].astype(f) + far[...].astype(f))
        m = m.astype(jnp.bfloat16)
        og[...] = m[:, :uw]
        ou[...] = m[:, uw:]

    @pl.when(meta[0] == 0)
    def _():
        store(far_b)

    @pl.when(meta[0] == 1)
    def _():
        store(far_a)


def mix_chunk(c, meta, own, near, far_a, far_b, done):
    width, both = own.shape
    uw = both // 2
    band = 512
    read = pl.BlockSpec((band, both), lambda i: (i, 0))
    write = pl.BlockSpec((band, uw), lambda i: (i, c))
    extra = [] if done is None else list(done)
    return pl.pallas_call(
        mix_body,
        grid=(width // band,),
        out_shape=(jax.ShapeDtypeStruct((width, CHUNKS * uw), jnp.bfloat16),) * 2,
        in_specs=[SMEM] + [read] * 4 + [ANY] * len(extra),
        out_specs=(write, write),
        input_output_aliases={} if done is None else {5: 0, 6: 1},
        compiler_params=params(10),
        name="mix",
    )(meta, own, near, far_a, far_b, *extra)


def local(tokens, hidden_grad, w_gate, w_up):
    axes = ("grp", "dp")
    groups = lax.axis_size("grp")
    own = tokens[0]
    dp = lax.axis_index("dp")
    core = lax.axis_index("grp") % 2
    z, x = dp // NX, dp % NX

    def send(v, move):
        return lax.ppermute(v, axes, device_pairs(groups, move))

    def along_x(v, by):
        return send(v, lambda g, u, t: (g, u, t + by))

    def along_z(v, by):
        return send(v, lambda g, u, t: (g, u + by, t))

    def table(pairs):
        up = jnp.array([k for k, d in pairs], jnp.int32)
        along = jnp.array([d for k, d in pairs], jnp.int32)
        src = ((z + NZ - up) % NZ) * NX + (x + NX - along) % NX
        return jnp.concatenate([core.reshape(1), src]).astype(jnp.int32)

    meta_a = table([(k, d) for k in range(NZ) for d in DX])
    meta_b = table([(k, d) for d in DX for k in range(NZ)])

    def fan(v):
        out = [v]
        for d in DX[1:]:
            out.append(along_x(v, d))
        return out

    def swap(v):
        return send(v, lambda g, u, t: (g + 1 - 2 * (g % 2), u, t))

    half_a, half_b = pick(meta_a, own, swap(own))
    w = pack_weights(w_gate[0], w_up[0])
    r1 = along_z(half_a, 1)
    own_a = fan(half_a)
    b1 = along_z(half_b, 1)
    r2 = along_z(r1, 1)
    one_a = fan(r1)
    b2 = along_z(b1, 1)
    r3 = along_z(r2, 1)
    hg = split_units(hidden_grad[0], NZ * NX)
    hg = lax.all_to_all(hg, "dp", split_axis=0, concat_axis=0, tiled=True)
    b3 = along_z(b2, 1)
    two_a = fan(r2)
    three_a = fan(r3)
    column_b = [b1, b2, b3]
    early = cat(own_a + one_a + two_a)
    late = cat(three_a)
    pieces = [early, late, swap(early), swap(late)]

    step_a, cross_a = [], []
    for c in range(CHUNKS):
        step_a.append(step_chunk(0, c, meta_a, hg, w, pieces))
        cross_a.append(send(step_a[c], lambda g, u, t: (g - 1, u, t)))

    blocks = cat(fan(cat([half_b] + column_b, step_a[0])))
    blocks = [blocks, swap(blocks)]
    mine, cross_b, near = [], [], []
    for c in range(CHUNKS):
        mine.append(step_chunk(1, c, meta_b, hg, w, blocks, step_a[c]))
        cross_b.append(send(mine[c], lambda g, u, t: (g + 1, u, t)))
        near.append(swap(mine[c]))

    done = None
    for c in range(CHUNKS):
        done = mix_chunk(c, meta_a, mine[c], near[c], cross_a[c], cross_b[c], done)
    return done[0][None], done[1][None]


def solution(mesh):
    in_specs = (
        P("grp", "dp", None),
        P("grp", "dp", None),
        P("grp", None, "dp"),
        P("grp", None, "dp"),
    )
    out_specs = (P("grp", None, "dp"), P("grp", None, "dp"))

    return jax.shard_map(local, mesh=mesh, in_specs=in_specs, out_specs=out_specs, check_vma=False)
```

```python
import functools

import jax
import jax.numpy as jnp
from jax import lax
from jax.experimental import pallas as pl
from jax.experimental.pallas import tpu as pltpu
from jax.sharding import PartitionSpec as P


NZ = 4
NX = 4
DX = (0, 1, -1, 2)
CHUNKS = 3
VMEM = pl.BlockSpec(memory_space=pltpu.VMEM)
SMEM = pl.BlockSpec(memory_space=pltpu.SMEM)
ANY = pl.BlockSpec(memory_space=pl.ANY)
HBM = pl.BlockSpec(memory_space=pltpu.HBM)
MIB = 1024 * 1024


def params(mib):
    return pltpu.CompilerParams(vmem_limit_bytes=mib * MIB)


def device_pairs(grp, move):
    out = []
    for g in range(grp):
        for z in range(NZ):
            for x in range(NX):
                to = move(g, z, x)
                if to is not None:
                    h, u, v = to
                    out.append(((g * NZ + z) * NX + x, ((h % grp) * NZ + u % NZ) * NX + v % NX))
    return out


def split_body(hg, out, sem):
    units = out.shape[2]
    for i in range(out.shape[0]):
        pltpu.make_async_copy(hg.at[:, i * units:(i + 1) * units], out.at[i], sem.at[i]).start()
    for i in range(out.shape[0]):
        pltpu.make_async_copy(hg.at[:, i * units:(i + 1) * units], out.at[i], sem.at[i]).wait()


def split_units(hg, parts):
    rows, width = hg.shape
    return pl.pallas_call(
        split_body,
        out_shape=jax.ShapeDtypeStruct((parts, rows, width // parts), hg.dtype),
        in_specs=[HBM],
        out_specs=HBM,
        scratch_shapes=[pltpu.SemaphoreType.DMA((parts,))],
        compiler_params=params(4),
        name="split",
    )(hg)


def pack_body(g, u, out):
    uw = g.shape[1]
    out[0, :, :uw] = g[...]
    out[0, :, uw:] = u[...]


def pack_weights(g, u):
    width, units = g.shape
    uw = units // CHUNKS
    read = pl.BlockSpec((width, uw), lambda c: (0, c))
    return pl.pallas_call(
        pack_body,
        grid=(CHUNKS,),
        out_shape=jax.ShapeDtypeStruct((CHUNKS, width, 2 * uw), g.dtype),
        in_specs=[read, read],
        out_specs=pl.BlockSpec((1, width, 2 * uw), lambda c: (c, 0, 0)),
        compiler_params=params(10),
        name="pack",
    )(g, u)


def pick_body(meta, own, got, a, b, sems):
    half = a.shape[0]
    for core in range(2):
        @pl.when(meta[0] == core)
        def _():
            at = pl.ds(core * half, half)
            ca = pltpu.make_async_copy((own if core == 0 else got).at[at], a, sems.at[0])
            cb = pltpu.make_async_copy((got if core == 0 else own).at[at], b, sems.at[1])
            ca.start()
            cb.start()
            ca.wait()
            cb.wait()


def pick(meta, own, got):
    shape = jax.ShapeDtypeStruct((own.shape[0] // 2, own.shape[1]), own.dtype)
    return pl.pallas_call(
        pick_body,
        out_shape=(shape, shape),
        in_specs=[SMEM, HBM, HBM],
        out_specs=(HBM, HBM),
        scratch_shapes=[pltpu.SemaphoreType.DMA((2,))],
        compiler_params=params(4),
        name="pick",
    )(meta, own, got)


def cat_body(count, *refs):
    xs, out, sems = refs[:count], refs[-2], refs[-1]
    copies, at = [], 0
    for i, v in enumerate(xs):
        copies.append(pltpu.make_async_copy(v, out.at[pl.ds(at, v.shape[0])], sems.at[i]))
        at += v.shape[0]
    for c in copies:
        c.start()
    for c in copies:
        c.wait()


def cat(xs, *deps):
    n = sum(v.shape[0] for v in xs)
    return pl.pallas_call(
        functools.partial(cat_body, len(xs)),
        out_shape=jax.ShapeDtypeStruct((n,) + xs[0].shape[1:], xs[0].dtype),
        in_specs=[HBM] * (len(xs) + len(deps)),
        out_specs=HBM,
        scratch_shapes=[pltpu.SemaphoreType.DMA((len(xs),))],
        compiler_params=params(4),
        name="cat",
    )(*xs, *deps)


def step_body(which, count, c, meta, units, packed, *refs):
    xs = refs[:count]
    rest = refs[count:]
    other = rest[0] if which == 1 else None
    out, x, w, hg, rows, sems = rest[-6:]
    uw = w.shape[1] // 2
    blk = hg.shape[1] // 2
    part = 512
    scale = w.shape[0] ** (-0.5)

    @pl.when(meta[0] == which)
    def _():
        weights = pltpu.make_async_copy(packed.at[c], w, sems.at[x.shape[0] // part])
        weights.start()
        cotangents = pltpu.make_async_copy(units.at[:, :, c * uw:(c + 1) * uw], hg, sems.at[x.shape[0] // part + 1])
        cotangents.start()
        at = 0
        for v in xs:
            done = 0
            while done < v.shape[0]:
                n = min(part - at % part, v.shape[0] - done)
                pltpu.make_async_copy(v.at[pl.ds(done, n)], x.at[pl.ds(at, n)], sems.at[at // part]).start()
                at += n
                done += n
        weights.wait()
        cotangents.wait()

        def products(i, carry):
            at = pl.multiple_of(i * part, part)
            here = x.at[pl.ds(at, part)]
            pltpu.make_async_copy(here, here, sems.at[i]).wait()
            half = pl.multiple_of(jnp.where(i < 2, which, 1 - which) * blk, blk)
            gu = jnp.dot(x[pl.ds(at, part), :], w[...], preferred_element_type=jnp.float32) * scale
            for j in range(part // blk):
                gate = gu[j * blk:(j + 1) * blk, :uw]
                up = gu[j * blk:(j + 1) * blk, uw:]
                upstream = hg[meta[1 + (i % 2) * (part // blk) + j], pl.ds(half, blk), :].astype(jnp.float32)
                sigma = jax.nn.sigmoid(gate)
                g = upstream * up * sigma * (1.0 + gate * (1.0 - sigma))
                u = upstream * gate * sigma
                to = pl.ds(pl.multiple_of(at + j * blk, blk), blk)
                rows[to, :uw] = g.astype(jnp.bfloat16)
                rows[to, uw:] = u.astype(jnp.bfloat16)
            return carry

        lax.fori_loop(0, x.shape[0] // part, products, 0)

        def band(i, carry):
            at = pl.multiple_of(i * part, part)
            grad = lax.dot_general(x[:, pl.ds(at, part)], rows[...], (((0,), (0,)), ((), ())), preferred_element_type=jnp.float32)
            old = w[pl.ds(at, part), :].astype(jnp.float32)
            out[pl.ds(at, part), :] = (old - 0.5 * (grad * scale)).astype(jnp.bfloat16)
            return carry

        lax.fori_loop(0, w.shape[0] // part, band, 0)

    @pl.when(meta[0] != which)
    def _():
        if other is None:
            out[...] = jnp.zeros(out.shape, out.dtype)
        else:
            pltpu.sync_copy(other, out)


def step_chunk(which, c, meta, hg, w, xs, *extra):
    width = w.shape[1]
    n = sum(v.shape[0] for v in xs)
    both = w.shape[2]
    return pl.pallas_call(
        functools.partial(step_body, which, len(xs), c),
        grid=(1,),
        out_shape=jax.ShapeDtypeStruct((width, both), jnp.bfloat16),
        in_specs=[SMEM] + [HBM] * (2 + len(xs) + len(extra)),
        out_specs=pl.BlockSpec((width, both), lambda i: (0, 0)),
        scratch_shapes=[
            pltpu.VMEM((n, width), jnp.bfloat16),
            pltpu.VMEM((width, both), jnp.bfloat16),
            pltpu.VMEM(hg.shape[:2] + (both // 2,), jnp.bfloat16),
            pltpu.VMEM((n, both), jnp.bfloat16),
            pltpu.SemaphoreType.DMA((n // 512 + 2,)),
        ],
        compiler_params=params(32),
        cost_estimate=pl.CostEstimate(flops=4 * n * width * both, bytes_accessed=n * width * 2, transcendentals=n * 128),
        name="step",
    )(meta, hg, w, *xs, *extra)


def mix_body(meta, own, near, far_a, far_b, *refs):
    og, ou = refs[-2:]
    uw = og.shape[1]
    f = jnp.float32

    def store(far):
        m = 0.5 * own[...].astype(f) + 0.25 * (near[...].astype(f) + far[...].astype(f))
        m = m.astype(jnp.bfloat16)
        og[...] = m[:, :uw]
        ou[...] = m[:, uw:]

    @pl.when(meta[0] == 0)
    def _():
        store(far_b)

    @pl.when(meta[0] == 1)
    def _():
        store(far_a)


def mix_chunk(c, meta, own, near, far_a, far_b, done):
    width, both = own.shape
    uw = both // 2
    band = 512
    read = pl.BlockSpec((band, both), lambda i, meta: (i, 0))
    read_a = pl.BlockSpec((band, both), lambda i, meta: (i * meta[0], 0))
    read_b = pl.BlockSpec((band, both), lambda i, meta: (i * (1 - meta[0]), 0))
    write = pl.BlockSpec((band, uw), lambda i, meta: (i, c))
    extra = [] if done is None else list(done)
    return pl.pallas_call(
        mix_body,
        grid_spec=pltpu.PrefetchScalarGridSpec(
            num_scalar_prefetch=1,
            grid=(width // band,),
            in_specs=[read, read, read_a, read_b] + [ANY] * len(extra),
            out_specs=(write, write),
        ),
        out_shape=(jax.ShapeDtypeStruct((width, CHUNKS * uw), jnp.bfloat16),) * 2,
        input_output_aliases={} if done is None else {5: 0, 6: 1},
        compiler_params=params(10),
        name="mix",
    )(meta, own, near, far_a, far_b, *extra)


def local(tokens, hidden_grad, w_gate, w_up):
    axes = ("grp", "dp")
    groups = lax.axis_size("grp")
    own = tokens[0]
    dp = lax.axis_index("dp")
    core = lax.axis_index("grp") % 2
    z, x = dp // NX, dp % NX

    def send(v, move):
        return lax.ppermute(v, axes, device_pairs(groups, move))

    def along_x(v, by):
        return send(v, lambda g, u, t: (g, u, t + by))

    def along_z(v, by):
        return send(v, lambda g, u, t: (g, u + by, t))

    def table(pairs):
        up = jnp.array([k for k, d in pairs], jnp.int32)
        along = jnp.array([d for k, d in pairs], jnp.int32)
        src = ((z + NZ - up) % NZ) * NX + (x + NX - along) % NX
        return jnp.concatenate([core.reshape(1), src]).astype(jnp.int32)

    meta_a = table([(k, d) for k in range(NZ) for d in DX])
    meta_b = table([(k, d) for d in DX for k in range(NZ)])

    def fan(v):
        out = [v]
        for d in DX[1:]:
            out.append(along_x(v, d))
        return out

    def swap(v):
        return send(v, lambda g, u, t: (g + 1 - 2 * (g % 2), u, t))

    half_a, half_b = pick(meta_a, own, swap(own))
    w = pack_weights(w_gate[0], w_up[0])
    r1 = along_z(half_a, 1)
    own_a = fan(half_a)
    b1 = along_z(half_b, 1)
    r2 = along_z(r1, 1)
    one_a = fan(r1)
    b2 = along_z(b1, 1)
    r3 = along_z(r2, 1)
    hg = split_units(hidden_grad[0], NZ * NX)
    hg = lax.all_to_all(hg, "dp", split_axis=0, concat_axis=0, tiled=True)
    b3 = along_z(b2, 1)
    two_a = fan(r2)
    three_a = fan(r3)
    column_b = [b1, b2, b3]
    early = cat(own_a + one_a + two_a)
    late = cat(three_a)
    pieces = [early, late, swap(early), swap(late)]

    step_a, cross_a = [], []
    for c in range(CHUNKS):
        step_a.append(step_chunk(0, c, meta_a, hg, w, pieces))
        cross_a.append(send(step_a[c], lambda g, u, t: (g - 1, u, t)))

    blocks = cat(fan(cat([half_b] + column_b, step_a[0])))
    blocks = [blocks, swap(blocks)]
    mine, cross_b, near = [], [], []
    for c in range(CHUNKS):
        mine.append(step_chunk(1, c, meta_b, hg, w, blocks, step_a[c]))
        cross_b.append(send(mine[c], lambda g, u, t: (g + 1, u, t)))
        near.append(swap(mine[c]))

    done = None
    for c in range(CHUNKS):
        done = mix_chunk(c, meta_a, mine[c], near[c], cross_a[c], cross_b[c], done)
    return done[0][None], done[1][None]


def solution(mesh):
    in_specs = (
        P("grp", "dp", None),
        P("grp", "dp", None),
        P("grp", None, "dp"),
        P("grp", None, "dp"),
    )
    out_specs = (P("grp", None, "dp"), P("grp", None, "dp"))

    return jax.shard_map(local, mesh=mesh, in_specs=in_specs, out_specs=out_specs, check_vma=False)
```
